256 devices in a mesh: gx: 4 (over y_lo, core), gz: 8 (over y_hi, x), ta: 8 (over z).
Axes of the slice: x: 4, y: 4 (y_hi: 2, y_lo: 2; y = y_hi * 2 + y_lo), z: 8, core: 2. Of those that a mesh axis runs over, the one named last changes fastest.
Arguments:
- links: float32 [4, 2, 3, 3, 32, 32, 512], P(None, None, None, None, 'ta', 'gz', 'gx'), may hold values from -1 to 1, as said below
Outputs:
- force: float32 [4, 2, 3, 3, 32, 32, 512], P(None, None, None, None, 'ta', 'gz', 'gx')
The draws below stay inside these ranges and needn't reach their ends.
Inputs may be any that keep to these rules, and one draw needn't show every extreme that they name: Every link matrix (real part links[mu, 0], imaginary part links[mu, 1]) is special unitary, up to float32 rounding.
All inputs are finite; a program needn't handle non-finite values.
Results may differ from the reference program's by a relative error of at most 0.0003.
Values sent between devices are 32-bit elements; how exact they have to be, the bound alone decides.
A program may use at most 64 MiB of HBM per device.

```python
import jax
import jax.numpy as jnp

NX = 16
NY = 32
NZ = 32
NT = 32
NXY = 512


def draw_links(key, part):
    sample = jax.random.normal(key, (2, 4, 3, 3, NT, NZ, NXY), jnp.float32)
    real0 = sample[0][:, 0]
    imag0 = sample[1][:, 0]
    length0 = jnp.maximum(jnp.sqrt(jnp.sum(real0 * real0 + imag0 * imag0, axis=1, keepdims=True)), 1e-06)
    real0 = real0 / length0
    imag0 = imag0 / length0
    real1 = sample[0][:, 1]
    imag1 = sample[1][:, 1]
    inner_real = jnp.sum(real0 * real1 + imag0 * imag1, axis=1, keepdims=True)
    inner_imag = jnp.sum(real0 * imag1 - imag0 * real1, axis=1, keepdims=True)
    real1 = real1 - (inner_real * real0 - inner_imag * imag0)
    imag1 = imag1 - (inner_real * imag0 + inner_imag * real0)
    length1 = jnp.maximum(jnp.sqrt(jnp.sum(real1 * real1 + imag1 * imag1, axis=1, keepdims=True)), 1e-06)
    real1 = real1 / length1
    imag1 = imag1 / length1
    real_cols = []
    imag_cols = []
    for column in range(3):
        next_col = (column + 1) % 3
        last_col = (column + 2) % 3
        cross_real = real0[:, next_col] * real1[:, last_col] - imag0[:, next_col] * imag1[:, last_col] - real0[:, last_col] * real1[:, next_col] + imag0[:, last_col] * imag1[:, next_col]
        cross_imag = real0[:, next_col] * imag1[:, last_col] + imag0[:, next_col] * real1[:, last_col] - real0[:, last_col] * imag1[:, next_col] - imag0[:, last_col] * real1[:, next_col]
        real_cols.append(cross_real)
        imag_cols.append(-cross_imag)
    real2 = jnp.stack(real_cols, axis=1)
    imag2 = jnp.stack(imag_cols, axis=1)
    real_rows = jnp.stack([real0, real1, real2], axis=1)
    imag_rows = jnp.stack([imag0, imag1, imag2], axis=1)
    return jnp.stack([real_rows, imag_rows], axis=1)


def setup_inputs(seed: int = 0) -> dict:
    seeds = jax.random.split(jax.random.key(seed), 2)
    links = draw_links(jax.random.fold_in(seeds[1], 71), 0)
    return dict(links=links)


COEFF = -1.9


def matprod(left, right):
    total = left[:, 0][:, None] * right[0][None, :]
    total = total + left[:, 1][:, None] * right[1][None, :]
    return total + left[:, 2][:, None] * right[2][None, :]


def complex_mul(left, right):
    return (matprod(left[0], right[0]) - matprod(left[1], right[1]),
            matprod(left[0], right[1]) + matprod(left[1], right[0]))


def dagger(matrix):
    return (jnp.swapaxes(matrix[0], 0, 1), -jnp.swapaxes(matrix[1], 0, 1))


def unit_step(direction, sign):
    offset = [0, 0, 0, 0]
    offset[direction] = sign
    return tuple(offset)


def joined(first_step, second_step):
    return tuple(first_step[position] + second_step[position] for position in range(4))


def gauge_force(fetch_link):
    blocks = []
    still = (0, 0, 0, 0)
    for direction in range(4):
        ahead = unit_step(direction, 1)
        summed = None
        for transverse in range(4):
            if transverse == direction:
                continue
            side_up = unit_step(transverse, 1)
            side_down = unit_step(transverse, -1)
            upper = complex_mul(complex_mul(fetch_link(transverse, ahead), dagger(fetch_link(direction, side_up))),
                                dagger(fetch_link(transverse, still)))
            lower = complex_mul(complex_mul(dagger(fetch_link(transverse, joined(ahead, side_down))),
                                            dagger(fetch_link(direction, side_down))),
                                fetch_link(transverse, side_down))
            staple = (upper[0] + lower[0], upper[1] + lower[1])
            summed = staple if summed is None else (summed[0] + staple[0], summed[1] + staple[1])
        loop_matrix = complex_mul(fetch_link(direction, still), summed)
        real_part = 0.5 * (loop_matrix[0] - jnp.swapaxes(loop_matrix[0], 0, 1))
        imag_part = 0.5 * (loop_matrix[1] + jnp.swapaxes(loop_matrix[1], 0, 1))
        trace_third = (loop_matrix[1][0, 0] + loop_matrix[1][1, 1] + loop_matrix[1][2, 2]) / 3.0
        identity = jnp.eye(3, dtype=jnp.float32).reshape((3, 3) + (1,) * trace_third.ndim)
        imag_part = imag_part - identity * trace_third
        blocks.append(COEFF * jnp.stack([real_part, imag_part], axis=0))
    return jnp.stack(blocks, axis=0)


def reference(links):
    lattice = links.reshape(links.shape[:6] + (NY, NX))

    def fetch_link(direction, offset):
        field = lattice[direction]
        field = jnp.roll(field, (-offset[0], -offset[1], -offset[2], -offset[3]), axis=(3, 4, 5, 6))
        return (field[0], field[1])

    return gauge_force(fetch_link).reshape(links.shape)
```

```python
import functools

import jax
import jax.numpy as jnp
from jax import lax
from jax.experimental import pallas as pl
from jax.experimental.pallas import tpu as pltpu
from jax.sharding import PartitionSpec as P

MESH = pl.DeviceIdType.MESH
COEFF = -1.9
NX = 16
ROWS = 16
LANES = 128

STEP = (4, 1, 16, 1)
AXIS = (0, 0, 1, 1)
COUNT = (4, 4, 8, 16)
GROUP = (4, 4, 8)
RING = ("ta", "gz", "gx")
PLANES = ((0, 3), (2, 3), (0, 2), (1, 3), (1, 2), (0, 1))


def comp(mu, part, i, j):
    return ((mu * 2 + part) * 3 + i) * 3 + j


def slot(step_dir, link_dir):
    return step_dir * 3 + (link_dir if link_dir < step_dir else link_dir - 1)


def others(direction):
    return [d for d in range(4) if d != direction]


def position(direction):
    iota = lax.broadcasted_iota(jnp.int32, (ROWS, LANES), AXIS[direction])
    return (iota // STEP[direction]) % COUNT[direction]


def turn(value, direction, steps):
    size = (ROWS, LANES)[AXIS[direction]]
    amount = (steps * STEP[direction]) % size
    if amount == 0:
        return value
    return pltpu.roll(value, amount, axis=AXIS[direction])


def pack(loads, buf, direction, high):
    where = position(direction)
    width = GROUP[direction]
    for first in range(0, len(loads), width):
        packed = None
        for j, load in enumerate(loads[first : first + width]):
            moved = turn(load(), direction, j - (width - 1) if high else j)
            packed = moved if packed is None else jnp.where(where == j, moved, packed)
        buf[first // width] = packed


def unpack(buf, index, direction, high):
    width = GROUP[direction]
    j = index % width
    return turn(buf[index // width], direction, width - 1 - j if high else -j)


def cmul(a, b, conj_a=False, conj_b=False):
    (ar, ai), (br, bi) = a, b
    sa = -1 if conj_a else 1
    sb = -1 if conj_b else 1
    return ([(1, ar * br), (-sa * sb, ai * bi)], [(sb, ar * bi), (sa, ai * br)])


def total(terms):
    terms = sorted(terms, key=lambda term: -term[0])
    result = None
    for sign, value in terms:
        if result is None:
            result = value if sign > 0 else -value
        else:
            result = result + value if sign > 0 else result - value
    return result


def dot3(pairs, conj_a=False, conj_b=False, parts="ri"):
    real, imag = [], []
    for a, b in pairs:
        (ar, ai), (br, bi) = a, b
        sa = -1 if conj_a else 1
        sb = -1 if conj_b else 1
        if "r" in parts:
            real += [(1, ar * br), (-sa * sb, ai * bi)]
        if "i" in parts:
            imag += [(sb, ar * bi), (sa, ai * br)]
    return (total(real) if real else None, total(imag) if imag else None)


OFF = ((0, 1), (0, 2), (1, 2))


def leaf(entry, trace):
    values = []
    for i, j in OFF:
        upper = entry(i, j, "ri")
        lower = entry(j, i, "ri")
        values.append(upper[0] - lower[0])
        values.append(upper[1] + lower[1])
    for i in range(2):
        values.append(entry(i, i, "i")[1] - trace)
    return values


def kernel(links_ref, out_ref, u, shifted, store, leaves, wmat, send1, recv1, send2, recv2,
           in_sem, s1, r1, s2, r2):
    fetch = [
        pltpu.make_async_copy(links_ref.at[pl.ds(mu * 18, 18)], u.at[pl.ds(mu * 18, 18)], in_sem.at[mu])
        for mu in range(4)
    ]
    for copy in fetch:
        copy.start()

    index = [lax.axis_index(name) for name in RING]
    size = [lax.axis_size(name) for name in RING]
    below = [{RING[d]: lax.rem(index[d] + size[d] - 1, size[d])} for d in range(3)]
    above = [{RING[d]: lax.rem(index[d] + 1, size[d])} for d in range(3)]
    barrier = pltpu.get_barrier_semaphore()
    for d in (1, 0, 2):
        pl.semaphore_signal(barrier, inc=1, device_id=below[d], device_id_type=MESH)
        pl.semaphore_signal(barrier, inc=1, device_id=above[d], device_id_type=MESH)
    for copy in fetch:
        copy.wait()

    def link(mu, part, i, j):
        return lambda: u[comp(mu, part, i, j)]

    for d in (1, 0, 2):
        loads = [link(nu, part, i, j) for nu in others(d) for part in range(2) for i in range(2) for j in range(3)]
        pack(loads, send1[d], d, high=False)
    pl.semaphore_wait(barrier, 6)
    down = [
        pltpu.make_async_remote_copy(
            src_ref=send1[d], dst_ref=recv1[d], send_sem=s1.at[d], recv_sem=r1.at[d],
            device_id=below[d], device_id_type=MESH,
        )
        for d in range(3)
    ]
    for d in (1, 0, 2):
        down[d].start()

    def make_w(plane, mu, nu):
        def body(v, carry):
            rows = pl.ds(pl.multiple_of(v * 8, 8), 8)

            def get(ref, base):
                return [[(ref[base + i * 3 + j, rows, :], ref[base + 9 + i * 3 + j, rows, :])
                         for j in range(3)] for i in range(3)]

            a = get(u, mu * 18)
            b = get(u, nu * 18)
            for i in range(3):
                for j in range(3):
                    real, imag = dot3([(b[k][i], a[k][j]) for k in range(3)], conj_a=True)
                    wmat[plane * 18 + i * 3 + j, rows, :] = real
                    wmat[plane * 18 + 9 + i * 3 + j, rows, :] = imag
            return carry

        lax.fori_loop(0, 2, body, 0)

    def shift_x():
        edge = position(3) == NX - 1
        for nu in others(3):
            base = slot(3, nu) * 18
            for c in range(18):
                value = u[nu * 18 + c]
                shifted[base + c] = jnp.where(
                    edge, pltpu.roll(value, NX - 1, axis=1), pltpu.roll(value, LANES - 1, axis=1)
                )

    def shift_split(d):
        edge = position(d) == COUNT[d] - 1
        for order, nu in enumerate(others(d)):
            base = slot(d, nu) * 18
            got = {}
            for part in range(2):
                for i in range(2):
                    for j in range(3):
                        where = order * 12 + (part * 2 + i) * 3 + j
                        local = turn(u[comp(nu, part, i, j)], d, -1)
                        value = jnp.where(edge, unpack(recv1[d], where, d, high=True), local)
                        got[part, i, j] = value
                        shifted[base + part * 9 + i * 3 + j] = value
            for j in range(3):
                p, q = (j + 1) % 3, (j + 2) % 3
                r0p, r0q, r1p, r1q = got[0, 0, p], got[0, 0, q], got[0, 1, p], got[0, 1, q]
                i0p, i0q, i1p, i1q = got[1, 0, p], got[1, 0, q], got[1, 1, p], got[1, 1, q]
                shifted[base + 6 + j] = r0p * r1q - i0p * i1q - r0q * r1p + i0q * i1p
                shifted[base + 15 + j] = r0q * i1p + i0q * r1p - r0p * i1q - i0p * r1q

    seen = set()

    def do_plane(plane, mu, nu):
        fresh_mu, fresh_nu = mu not in seen, nu not in seen
        seen.update((mu, nu))

        def body(v, carry):
            rows = pl.ds(pl.multiple_of(v * 8, 8), 8)

            def get(ref, base, i, j):
                return (ref[base + i * 3 + j, rows, :], ref[base + 9 + i * 3 + j, rows, :])

            cbase = slot(mu, nu) * 18
            dbase = slot(nu, mu) * 18
            t = [[None] * 3 for _ in range(3)]
            for i in range(3):
                ci = [get(shifted, cbase, i, k) for k in range(3)]
                for j in range(3):
                    t[i][j] = dot3([(ci[k], get(shifted, dbase, j, k)) for k in range(3)], conj_b=True)

            x = [[None] * 3 for _ in range(3)]
            for i in range(3):
                ai = [get(u, mu * 18, i, k) for k in range(3)]
                for j in range(3):
                    x[i][j] = dot3([(ai[k], t[k][j]) for k in range(3)])

            def p_entry(i, j, parts):
                return dot3([(x[i][k], get(u, nu * 18, j, k)) for k in range(3)], conj_b=True, parts=parts)

            diag = [p_entry(i, i, "i")[1] for i in range(3)]
            trace = (diag[0] + diag[1] + diag[2]) * (1.0 / 3.0)
            values = leaf(lambda i, j, parts: (None, diag[i]) if i == j else p_entry(i, j, parts), trace)
            for c in range(8):
                at_mu = (mu * 8 + c, rows, slice(None))
                at_nu = (nu * 8 + c, rows, slice(None))
                if fresh_mu:
                    store[at_mu] = values[c]
                else:
                    store[at_mu] = store[at_mu] + values[c]
                if fresh_nu:
                    store[at_nu] = -values[c]
                else:
                    store[at_nu] = store[at_nu] - values[c]

            def w(i, j):
                return get(wmat, plane * 18, i, j)

            values = leaf(lambda i, j, parts: dot3([(w(i, k), t[k][j]) for k in range(3)], parts=parts), trace)
            for c in range(8):
                leaves[slot(nu, mu) * 8 + c, rows, :] = values[c]
            values = leaf(lambda i, j, parts: dot3([(t[i][k], w(k, j)) for k in range(3)], parts=parts), trace)
            for c in range(8):
                leaves[slot(mu, nu) * 8 + c, rows, :] = values[c]
            return carry

        lax.fori_loop(0, 2, body, 0)

    shift_x()
    for plane, (mu, nu) in enumerate(PLANES):
        make_w(plane, mu, nu)
    down[2].wait_recv()
    shift_split(2)
    do_plane(1, 2, 3)
    down[0].wait_recv()
    shift_split(0)
    do_plane(0, 0, 3)
    do_plane(2, 0, 2)
    down[1].wait_recv()
    shift_split(1)
    do_plane(3, 1, 3)
    do_plane(4, 1, 2)
    do_plane(5, 0, 1)

    up = [
        pltpu.make_async_remote_copy(
            src_ref=send2[d], dst_ref=recv2[d], send_sem=s2.at[d], recv_sem=r2.at[d],
            device_id=above[d], device_id_type=MESH,
        )
        for d in range(3)
    ]

    def leaf_at(index):
        return lambda: leaves[index]

    for d in (1, 0, 2):
        pack([leaf_at(slot(d, nu) * 8 + c) for nu in others(d) for c in range(8)], send2[d], d, high=True)
    for d in (1, 0, 2):
        up[d].start()

    def sign(d, nu):
        return -1 if (nu, d) in PLANES else 1

    def add(at, value, positive):
        store[at] = store[at] + value if positive else store[at] - value

    first = position(3) == 0
    for nu in others(3):
        for c in range(8):
            value = leaves[slot(3, nu) * 8 + c]
            value = jnp.where(first, pltpu.roll(value, LANES - NX + 1, axis=1), pltpu.roll(value, 1, axis=1))
            add(nu * 8 + c, value, sign(3, nu) > 0)
    for d in (2, 0, 1):
        up[d].wait_recv()
        first = position(d) == 0
        for order, nu in enumerate(others(d)):
            for c in range(8):
                value = turn(leaves[slot(d, nu) * 8 + c], d, 1)
                value = jnp.where(first, unpack(recv2[d], order * 8 + c, d, high=False), value)
                add(nu * 8 + c, value, sign(d, nu) > 0)

    for mu in range(4):
        for number, (i, j) in enumerate(OFF):
            real = store[mu * 8 + number * 2] * (0.5 * COEFF)
            imag = store[mu * 8 + number * 2 + 1] * (0.5 * COEFF)
            out_ref[comp(mu, 0, i, j)] = real
            out_ref[comp(mu, 0, j, i)] = -real
            out_ref[comp(mu, 1, i, j)] = imag
            out_ref[comp(mu, 1, j, i)] = imag
        diag0 = store[mu * 8 + 6] * COEFF
        diag1 = store[mu * 8 + 7] * COEFF
        for i, value in enumerate((diag0, diag1, -(diag0 + diag1))):
            out_ref[comp(mu, 1, i, i)] = value
            out_ref[comp(mu, 0, i, i)] = jnp.zeros_like(value)

    for d in range(3):
        down[d].wait_send()
        up[d].wait_send()


def per_device(links):
    shape = links.shape
    vmem = pltpu.VMEM
    counts1 = [-(-36 // g) for g in GROUP]
    counts2 = [24 // g for g in GROUP]

    def packed(counts):
        return [vmem((n, ROWS, LANES), jnp.float32) for n in counts]

    out = pl.pallas_call(
        kernel,
        out_shape=jax.ShapeDtypeStruct((72, ROWS, LANES), jnp.float32),
        in_specs=[pl.BlockSpec(memory_space=pl.ANY)],
        out_specs=pl.BlockSpec(memory_space=pltpu.VMEM),
        scratch_shapes=[
            vmem((72, ROWS, LANES), jnp.float32),
            vmem((216, ROWS, LANES), jnp.float32),
            vmem((32, ROWS, LANES), jnp.float32),
            vmem((96, ROWS, LANES), jnp.float32),
            vmem((108, ROWS, LANES), jnp.float32),
            packed(counts1),
            packed(counts1),
            packed(counts2),
            packed(counts2),
            pltpu.SemaphoreType.DMA((4,)),
            pltpu.SemaphoreType.DMA((3,)),
            pltpu.SemaphoreType.DMA((3,)),
            pltpu.SemaphoreType.DMA((3,)),
            pltpu.SemaphoreType.DMA((3,)),
        ],
        compiler_params=pltpu.CompilerParams(collective_id=0, has_side_effects=True),
    )(links.reshape(72, ROWS, LANES))
    return out.reshape(shape)


def solution(mesh):
    return jax.shard_map(
        per_device,
        mesh=mesh,
        in_specs=(P(None, None, None, None, "ta", "gz", "gx"),),
        out_specs=P(None, None, None, None, "ta", "gz", "gx"),
        check_vma=False,
    )
```

```python
import functools

import jax
import jax.numpy as jnp
from jax import lax
from jax.experimental import pallas as pl
from jax.experimental.pallas import tpu as pltpu
from jax.sharding import PartitionSpec as P

MESH = pl.DeviceIdType.MESH
COEFF = -1.9
NX = 16
ROWS = 16
LANES = 128

STEP = (4, 1, 16, 1)
AXIS = (0, 0, 1, 1)
COUNT = (4, 4, 8, 16)
GROUP = (4, 4, 8)
RING = ("ta", "gz", "gx")
PLANES = ((0, 3), (2, 3), (0, 2), (1, 3), (1, 2), (0, 1))


def comp(mu, part, i, j):
    return ((mu * 2 + part) * 3 + i) * 3 + j


def slot(step_dir, link_dir):
    return step_dir * 3 + (link_dir if link_dir < step_dir else link_dir - 1)


def others(direction):
    return [d for d in range(4) if d != direction]


def position(direction):
    iota = lax.broadcasted_iota(jnp.int32, (ROWS, LANES), AXIS[direction])
    return (iota // STEP[direction]) % COUNT[direction]


def turn(value, direction, steps):
    size = (ROWS, LANES)[AXIS[direction]]
    amount = (steps * STEP[direction]) % size
    if amount == 0:
        return value
    return pltpu.roll(value, amount, axis=AXIS[direction])


def pack(loads, buf, direction, high):
    where = position(direction)
    width = GROUP[direction]
    for first in range(0, len(loads), width):
        packed = None
        for j, load in enumerate(loads[first : first + width]):
            moved = turn(load(), direction, j - (width - 1) if high else j)
            packed = moved if packed is None else jnp.where(where == j, moved, packed)
        buf[first // width] = packed


def unpack(buf, index, direction, high):
    width = GROUP[direction]
    j = index % width
    return turn(buf[index // width], direction, width - 1 - j if high else -j)


def edge_place(d, e, c):
    return (c // 8, c % 8) if e == 2 else (c % 4, c // 4)


def pack_edge(loads, buf, d, e):
    packed = None
    for c, load in enumerate(loads):
        at_d, at_e = edge_place(d, e, c)
        moved = turn(turn(load(), d, at_d - (COUNT[d] - 1)), e, at_e)
        here = (position(d) == at_d) & (position(e) == at_e)
        packed = moved if packed is None else jnp.where(here, moved, packed)
    buf[...] = packed


def unpack_edge(buf, d, e, c, to_d):
    at_d, at_e = edge_place(d, e, c)
    return turn(turn(buf[...], d, to_d - at_d), e, COUNT[e] - 1 - at_e)


def shift_within_x(value):
    edge = position(3) == NX - 1
    return jnp.where(edge, pltpu.roll(value, NX - 1, axis=1), pltpu.roll(value, LANES - 1, axis=1))


def third_row(get, put):
    for j in range(3):
        p, q = (j + 1) % 3, (j + 2) % 3
        r0p, r0q, r1p, r1q = get(0, 0, p), get(0, 0, q), get(0, 1, p), get(0, 1, q)
        i0p, i0q, i1p, i1q = get(1, 0, p), get(1, 0, q), get(1, 1, p), get(1, 1, q)
        put(0, j, r0p * r1q - i0p * i1q - r0q * r1p + i0q * i1p)
        put(1, j, r0q * i1p + i0q * r1p - r0p * i1q - i0p * r1q)


def total(terms):
    terms = sorted(terms, key=lambda term: -term[0])
    result = None
    for sign, value in terms:
        if result is None:
            result = value if sign > 0 else -value
        else:
            result = result + value if sign > 0 else result - value
    return result


def dot3(pairs, conj_a=False, conj_b=False, parts="ri"):
    real, imag = [], []
    for a, b in pairs:
        (ar, ai), (br, bi) = a, b
        sa = -1 if conj_a else 1
        sb = -1 if conj_b else 1
        if "r" in parts:
            real += [(1, ar * br), (-sa * sb, ai * bi)]
        if "i" in parts:
            imag += [(sb, ar * bi), (sa, ai * br)]
    return (total(real) if real else None, total(imag) if imag else None)


OFF = ((0, 1), (0, 2), (1, 2))


def leaf(entry, trace):
    values = []
    for i, j in OFF:
        upper = entry(i, j, "ri")
        lower = entry(j, i, "ri")
        values.append(upper[0] - lower[0])
        values.append(upper[1] + lower[1])
    for i in range(2):
        values.append(entry(i, i, "i")[1] - trace)
    return values


FACES = (0, 1)
EDGES = ((0, 1), (0, 2), (1, 0), (1, 2))
OUTGOING = (
    [tuple(-1 if k == d else 0 for k in range(3)) for d in range(3)]
    + [tuple(1 if k == d else 0 for k in range(3)) for d in range(3)]
    + [tuple(1 if k == d else -1 if k == e else 0 for k in range(3)) for d, e in EDGES]
)
TWO_ROWS = [(part, i, j) for part in range(2) for i in range(2) for j in range(3)]


def kernel(links_ref, out_ref, u, shifted, store, leaves, wmat, send1, recv1, send2, recv2, sende, recve,
           near, far, base, moved, faceleaf, in_sem, s1, r1, s2, r2, se, re):
    index = [lax.axis_index(name) for name in RING]
    size = [lax.axis_size(name) for name in RING]
    first_time = index[0] == 0
    last_time = index[0] == size[0] - 1

    def device(offset, back=False):
        return {
            RING[k]: lax.rem(index[k] + size[k] + (-step if back else step), size[k])
            for k, step in enumerate(offset)
            if step
        }

    barrier = pltpu.get_barrier_semaphore()

    def greet(offset):
        pl.semaphore_signal(barrier, inc=1, device_id=device(offset, back=True), device_id_type=MESH)

    fetch = [
        pltpu.make_async_copy(links_ref.at[pl.ds(mu * 18, 18)], u.at[pl.ds(mu * 18, 18)], in_sem.at[mu])
        for mu in range(4)
    ]
    for copy in fetch:
        copy.start()

    for offset in OUTGOING:
        if offset[0] == 0:
            greet(offset)

    @pl.when(jnp.logical_not(first_time))
    def _():
        for offset in OUTGOING:
            if offset[0] == 1:
                greet(offset)

    @pl.when(jnp.logical_not(last_time))
    def _():
        for offset in OUTGOING:
            if offset[0] == -1:
                greet(offset)

    for copy in fetch:
        copy.wait()

    def link(mu, part, i, j):
        return lambda: u[comp(mu, part, i, j)]

    for d in FACES:
        pack([link(nu, *c) for c in TWO_ROWS for nu in others(d) + [d]], send2[d], d, high=True)
    for number, (d, e) in enumerate(EDGES):
        pack_edge([link(d, *c) for c in TWO_ROWS], sende[number], d, e)
    for d in (1, 0, 2):
        pack([link(nu, *c) for nu in others(d) for c in TWO_ROWS], send1[d], d, high=False)

    down_time = [offset for offset in OUTGOING if offset[0] == -1]

    @pl.when(first_time)
    def _():
        pl.semaphore_wait(barrier, len(OUTGOING) - len(down_time))
        for offset in OUTGOING:
            if offset[0] == 1:
                greet(offset)

    @pl.when(jnp.logical_not(first_time))
    def _():
        pl.semaphore_wait(barrier, len(OUTGOING))

    @pl.when(last_time)
    def _():
        for offset in down_time:
            greet(offset)

    def remote(src, dst, send, recv, offset):
        return pltpu.make_async_remote_copy(
            src_ref=src, dst_ref=dst, send_sem=send, recv_sem=recv,
            device_id=device(offset), device_id_type=MESH,
        )

    down = [remote(send1[d], recv1[d], s1.at[d], r1.at[d], OUTGOING[d]) for d in range(3)]
    up = [remote(send2[d], recv2[d], s2.at[d], r2.at[d], OUTGOING[3 + d]) for d in range(3)]
    corner = [remote(sende[n], recve[n], se.at[n], re.at[n], OUTGOING[6 + n]) for n in range(4)]
    up[0].start()
    up[1].start()
    down[1].start()
    down[2].start()
    for n in (0, 1, 3):
        corner[n].start()

    @pl.when(jnp.logical_not(first_time))
    def _():
        down[0].start()
        corner[2].start()

    def make_w(plane, mu, nu):
        def body(v, carry):
            rows = pl.ds(pl.multiple_of(v * 8, 8), 8)

            def get(ref, base):
                return [[(ref[base + i * 3 + j, rows, :], ref[base + 9 + i * 3 + j, rows, :])
                         for j in range(3)] for i in range(3)]

            a = get(u, mu * 18)
            b = get(u, nu * 18)
            for i in range(3):
                for j in range(3):
                    real, imag = dot3([(b[k][i], a[k][j]) for k in range(3)], conj_a=True)
                    wmat[plane * 18 + i * 3 + j, rows, :] = real
                    wmat[plane * 18 + 9 + i * 3 + j, rows, :] = imag
            return carry

        lax.fori_loop(0, 2, body, 0)

    def shift_x():
        for nu in others(3):
            at = slot(3, nu) * 18
            for c in range(18):
                shifted[at + c] = shift_within_x(u[nu * 18 + c])

    def shift_split(d):
        edge = position(d) == COUNT[d] - 1
        for order, nu in enumerate(others(d)):
            at = slot(d, nu) * 18
            got = {}
            for number, (part, i, j) in enumerate(TWO_ROWS):
                local = turn(u[comp(nu, part, i, j)], d, -1)
                value = jnp.where(edge, unpack(recv1[d], order * 12 + number, d, high=True), local)
                got[part, i, j] = value
                shifted[at + part * 9 + i * 3 + j] = value

            def put(part, j, value, at=at):
                shifted[at + part * 9 + 6 + j] = value

            third_row(lambda *c: got[c], put)

    def face_near(d):
        where = position(d)
        for c in range(18):
            value = None
            for j, nu in enumerate(others(d)):
                part = turn(u[nu * 18 + c], d, j)
                value = part if value is None else jnp.where(where == j, part, value)
            near[d * 18 + c] = value

    def face_leaf(d):
        where = position(d)
        got_far, got_base, got_moved = {}, {}, {}
        for number, c in enumerate(TWO_ROWS):
            value = recv2[d][number]
            got_far[c] = value
            spread = value
            for j in range(3):
                spread = jnp.where(where == j, turn(value, d, j - 3), spread)
            got_base[c] = spread
            shift = shift_within_x(spread)
            for j, mu in enumerate(others(d)):
                if mu == 3:
                    continue
                edge = EDGES.index((d, mu))
                step = jnp.where(
                    position(mu) == COUNT[mu] - 1,
                    unpack_edge(recve[edge], d, mu, number, j),
                    turn(spread, mu, -1),
                )
                shift = jnp.where(where == j, step, shift)
            got_moved[c] = shift
        for ref, got in ((far, got_far), (base, got_base), (moved, got_moved)):
            for (part, i, j), value in got.items():
                ref[part * 9 + i * 3 + j] = value

            def put(part, j, value, ref=ref):
                ref[part * 9 + 6 + j] = value

            third_row(lambda *c: got[c], put)

        def body(v, carry):
            rows = pl.ds(pl.multiple_of(v * 8, 8), 8)

            def get(ref, at, i, j):
                return (ref[at + i * 3 + j, rows, :], ref[at + 9 + i * 3 + j, rows, :])

            g = [[None] * 3 for _ in range(3)]
            for i in range(3):
                hi = [get(far, 0, i, k) for k in range(3)]
                for j in range(3):
                    g[i][j] = dot3([(hi[k], get(moved, 0, k, j)) for k in range(3)])
            x = [[None] * 3 for _ in range(3)]
            for i in range(3):
                ai = [get(near, d * 18, i, k) for k in range(3)]
                for j in range(3):
                    x[i][j] = dot3([(ai[k], g[j][k]) for k in range(3)], conj_b=True)

            def entry(i, j, parts):
                return dot3([(x[i][k], get(base, 0, k, j)) for k in range(3)], parts=parts)

            diag = [entry(i, i, "i")[1] for i in range(3)]
            trace = (diag[0] + diag[1] + diag[2]) * (1.0 / 3.0)
            values = leaf(lambda i, j, parts: (None, diag[i]) if i == j else entry(i, j, parts), trace)
            for c in range(8):
                faceleaf[c, rows, :] = values[c]
            return carry

        lax.fori_loop(0, 2, body, 0)

    seen = set()

    def do_plane(plane, mu, nu):
        fresh_mu, fresh_nu = mu not in seen, nu not in seen
        seen.update((mu, nu))

        def body(v, carry):
            rows = pl.ds(pl.multiple_of(v * 8, 8), 8)

            def get(ref, base, i, j):
                return (ref[base + i * 3 + j, rows, :], ref[base + 9 + i * 3 + j, rows, :])

            cbase = slot(mu, nu) * 18
            dbase = slot(nu, mu) * 18
            t = [[None] * 3 for _ in range(3)]
            for i in range(3):
                ci = [get(shifted, cbase, i, k) for k in range(3)]
                for j in range(3):
                    t[i][j] = dot3([(ci[k], get(shifted, dbase, j, k)) for k in range(3)], conj_b=True)

            x = [[None] * 3 for _ in range(3)]
            for i in range(3):
                ai = [get(u, mu * 18, i, k) for k in range(3)]
                for j in range(3):
                    x[i][j] = dot3([(ai[k], t[k][j]) for k in range(3)])

            def p_entry(i, j, parts):
                return dot3([(x[i][k], get(u, nu * 18, j, k)) for k in range(3)], conj_b=True, parts=parts)

            diag = [p_entry(i, i, "i")[1] for i in range(3)]
            trace = (diag[0] + diag[1] + diag[2]) * (1.0 / 3.0)
            values = leaf(lambda i, j, parts: (None, diag[i]) if i == j else p_entry(i, j, parts), trace)
            for c in range(8):
                at_mu = (mu * 8 + c, rows, slice(None))
                at_nu = (nu * 8 + c, rows, slice(None))
                if fresh_mu:
                    store[at_mu] = values[c]
                else:
                    store[at_mu] = store[at_mu] + values[c]
                if fresh_nu:
                    store[at_nu] = -values[c]
                else:
                    store[at_nu] = store[at_nu] - values[c]

            def w(i, j):
                return get(wmat, plane * 18, i, j)

            values = leaf(lambda i, j, parts: dot3([(w(i, k), t[k][j]) for k in range(3)], parts=parts), trace)
            for c in range(8):
                leaves[slot(nu, mu) * 8 + c, rows, :] = values[c]
            values = leaf(lambda i, j, parts: dot3([(t[i][k], w(k, j)) for k in range(3)], parts=parts), trace)
            for c in range(8):
                leaves[slot(mu, nu) * 8 + c, rows, :] = values[c]
            return carry

        lax.fori_loop(0, 2, body, 0)

    shift_x()
    for plane, (mu, nu) in enumerate(PLANES):
        make_w(plane, mu, nu)
    for d in FACES:
        face_near(d)
    down[2].wait_recv()
    shift_split(2)
    do_plane(1, 2, 3)
    down[1].wait_recv()
    shift_split(1)
    do_plane(4, 1, 2)
    do_plane(3, 1, 3)
    down[0].wait_recv()
    shift_split(0)
    do_plane(2, 0, 2)

    def leaf_at(index):
        return lambda: leaves[index]

    pack([leaf_at(slot(2, nu) * 8 + c) for nu in others(2) for c in range(8)], send2[2], 2, high=True)
    do_plane(0, 0, 3)
    up[2].start()
    do_plane(5, 0, 1)

    @pl.when(first_time)
    def _():
        pl.semaphore_wait(barrier, len(down_time))
        down[0].start()
        corner[2].start()

    def sign(d, nu):
        return -1 if (nu, d) in PLANES else 1

    def add(at, value, positive):
        store[at] = store[at] + value if positive else store[at] - value

    first = position(3) == 0
    for nu in others(3):
        for c in range(8):
            value = leaves[slot(3, nu) * 8 + c]
            value = jnp.where(first, pltpu.roll(value, LANES - NX + 1, axis=1), pltpu.roll(value, 1, axis=1))
            add(nu * 8 + c, value, sign(3, nu) > 0)
    up[2].wait_recv()
    first = position(2) == 0
    for order, nu in enumerate(others(2)):
        for c in range(8):
            value = turn(leaves[slot(2, nu) * 8 + c], 2, 1)
            value = jnp.where(first, unpack(recv2[2], order * 8 + c, 2, high=False), value)
            add(nu * 8 + c, value, sign(2, nu) > 0)
    for d in (1, 0):
        up[d].wait_recv()
        for n, (first, _) in enumerate(EDGES):
            if first == d:
                corner[n].wait_recv()
        face_leaf(d)
        first = position(d) == 0
        for order, nu in enumerate(others(d)):
            for c in range(8):
                value = turn(leaves[slot(d, nu) * 8 + c], d, 1)
                edge = turn(faceleaf[c], d, -order)
                add(nu * 8 + c, jnp.where(first, edge if sign(d, nu) > 0 else -edge, value), sign(d, nu) > 0)

    for mu in range(4):
        for number, (i, j) in enumerate(OFF):
            real = store[mu * 8 + number * 2] * (0.5 * COEFF)
            imag = store[mu * 8 + number * 2 + 1] * (0.5 * COEFF)
            out_ref[comp(mu, 0, i, j)] = real
            out_ref[comp(mu, 0, j, i)] = -real
            out_ref[comp(mu, 1, i, j)] = imag
            out_ref[comp(mu, 1, j, i)] = imag
        diag0 = store[mu * 8 + 6] * COEFF
        diag1 = store[mu * 8 + 7] * COEFF
        for i, value in enumerate((diag0, diag1, -(diag0 + diag1))):
            out_ref[comp(mu, 1, i, i)] = value
            out_ref[comp(mu, 0, i, i)] = jnp.zeros_like(value)

    for copy in down + up + corner:
        copy.wait_send()


def per_device(links):
    shape = links.shape
    vmem = pltpu.VMEM

    def packed(counts):
        return [vmem((n, ROWS, LANES), jnp.float32) for n in counts]

    counts1 = [-(-36 // g) for g in GROUP]
    counts2 = (12, 12, 3)
    edges = [vmem((ROWS, LANES), jnp.float32) for _ in EDGES]
    arrays = (72, 216, 32, 96, 108)
    dma = pltpu.SemaphoreType.DMA
    out = pl.pallas_call(
        kernel,
        out_shape=jax.ShapeDtypeStruct((72, ROWS, LANES), jnp.float32),
        in_specs=[pl.BlockSpec(memory_space=pltpu.HBM)],
        out_specs=pl.BlockSpec(memory_space=pltpu.VMEM),
        scratch_shapes=packed(arrays)
        + [packed(counts1), packed(counts1), packed(counts2), packed(counts2), edges, edges]
        + packed((36, 18, 18, 18, 8))
        + [dma((n,)) for n in (4, 3, 3, 3, 3, 4, 4)],
        compiler_params=pltpu.CompilerParams(
            collective_id=0, has_side_effects=True, vmem_limit_bytes=16 * 1024 * 1024
        ),
    )(pltpu.with_memory_space_constraint(links.reshape(72, ROWS, LANES), pltpu.HBM))
    return out.reshape(shape)


def solution(mesh):
    return jax.shard_map(
        per_device,
        mesh=mesh,
        in_specs=(P(None, None, None, None, "ta", "gz", "gx"),),
        out_specs=P(None, None, None, None, "ta", "gz", "gx"),
        check_vma=False,
    )
```

```python
import functools

import jax
import jax.numpy as jnp
from jax import lax
from jax.experimental import pallas as pl
from jax.experimental.pallas import tpu as pltpu
from jax.sharding import PartitionSpec as P

MESH = pl.DeviceIdType.MESH
COEFF = -1.9
NX = 16
ROWS = 16
LANES = 128

STEP = (4, 1, 16, 1)
AXIS = (0, 0, 1, 1)
COUNT = (4, 4, 8, 16)
GROUP = (4, 4, 8)
RING = ("ta", "gz", "gx")
PLANES = ((0, 3), (2, 3), (0, 2), (1, 3), (1, 2), (0, 1))


def comp(mu, part, i, j):
    return ((mu * 2 + part) * 3 + i) * 3 + j


def slot(step_dir, link_dir):
    return step_dir * 3 + (link_dir if link_dir < step_dir else link_dir - 1)


def others(direction):
    return [d for d in range(4) if d != direction]


def position(direction):
    iota = lax.broadcasted_iota(jnp.int32, (ROWS, LANES), AXIS[direction])
    return (iota // STEP[direction]) % COUNT[direction]


def turn(value, direction, steps):
    size = (ROWS, LANES)[AXIS[direction]]
    amount = (steps * STEP[direction]) % size
    if amount == 0:
        return value
    return pltpu.roll(value, amount, axis=AXIS[direction])


def pack(loads, buf, direction, high):
    where = position(direction)
    width = GROUP[direction]
    for first in range(0, len(loads), width):
        packed = None
        for j, load in enumerate(loads[first : first + width]):
            moved = turn(load(), direction, j - (width - 1) if high else j)
            packed = moved if packed is None else jnp.where(where == j, moved, packed)
        buf[first // width] = packed


def unpack(buf, index, direction, high):
    width = GROUP[direction]
    j = index % width
    return turn(buf[index // width], direction, width - 1 - j if high else -j)


def edge_place(d, e, c):
    return (c // 8, c % 8) if e == 2 else (c % 4, c // 4)


def pack_edge(loads, buf, d, e):
    packed = None
    for c, load in enumerate(loads):
        at_d, at_e = edge_place(d, e, c)
        moved = turn(turn(load(), d, at_d - (COUNT[d] - 1)), e, at_e)
        here = (position(d) == at_d) & (position(e) == at_e)
        packed = moved if packed is None else jnp.where(here, moved, packed)
    buf[...] = packed


def unpack_edge(buf, d, e, c, to_d):
    at_d, at_e = edge_place(d, e, c)
    return turn(turn(buf[...], d, to_d - at_d), e, COUNT[e] - 1 - at_e)


def shift_within_x(value):
    edge = position(3) == NX - 1
    return jnp.where(edge, pltpu.roll(value, NX - 1, axis=1), pltpu.roll(value, LANES - 1, axis=1))


def third_row(get, put):
    for j in range(3):
        p, q = (j + 1) % 3, (j + 2) % 3
        r0p, r0q, r1p, r1q = get(0, 0, p), get(0, 0, q), get(0, 1, p), get(0, 1, q)
        i0p, i0q, i1p, i1q = get(1, 0, p), get(1, 0, q), get(1, 1, p), get(1, 1, q)
        put(0, j, r0p * r1q - i0p * i1q - r0q * r1p + i0q * i1p)
        put(1, j, r0q * i1p + i0q * r1p - r0p * i1q - i0p * r1q)


def total(terms):
    terms = sorted(terms, key=lambda term: -term[0])
    result = None
    for sign, value in terms:
        if result is None:
            result = value if sign > 0 else -value
        else:
            result = result + value if sign > 0 else result - value
    return result


def dot3(pairs, conj_a=False, conj_b=False, parts="ri"):
    real, imag = [], []
    for a, b in pairs:
        (ar, ai), (br, bi) = a, b
        sa = -1 if conj_a else 1
        sb = -1 if conj_b else 1
        if "r" in parts:
            real += [(1, ar * br), (-sa * sb, ai * bi)]
        if "i" in parts:
            imag += [(sb, ar * bi), (sa, ai * br)]
    return (total(real) if real else None, total(imag) if imag else None)


OFF = ((0, 1), (0, 2), (1, 2))


def leaf(entry, trace):
    values = []
    for i, j in OFF:
        upper = entry(i, j, "ri")
        lower = entry(j, i, "ri")
        values.append(upper[0] - lower[0])
        values.append(upper[1] + lower[1])
    for i in range(2):
        values.append(entry(i, i, "i")[1] - trace)
    return values


FACES = (0, 1, 2)
EDGES = ((0, 1), (0, 2), (1, 0), (1, 2), (2, 0), (2, 1))


def offset_of(plus=None, minus=None):
    return tuple(1 if k == plus else -1 if k == minus else 0 for k in range(3))


DOWN = [offset_of(minus=d) for d in range(3)]
UP = [offset_of(plus=d) for d in range(3)]
CORNER = [offset_of(d, e) for d, e in EDGES]
DIRECT = [EDGES.index(pair) for pair in ((1, 0), (1, 2), (2, 0))]
OUTGOING = DOWN + UP + [CORNER[n] for n in DIRECT]
WRAP_LATER = [CORNER[EDGES.index(pair)] for pair in ((1, 0), (2, 0))]
WRAP_SOONER = [CORNER[EDGES.index(pair)] for pair in ((0, 1), (0, 2))]
TWO_ROWS = [(part, i, j) for part in range(2) for i in range(2) for j in range(3)]


def kernel(links_ref, out_ref, u, shifted, store, leaves, wmat, send1, recv1, send2, recv2, sende, recve,
           near, far, base, moved, faceleaf, in_sem, s1, r1, s2, r2, se, re):
    index = [lax.axis_index(name) for name in RING]
    size = [lax.axis_size(name) for name in RING]
    first_time = index[0] == 0
    last_time = index[0] == size[0] - 1

    def device(offset, back=False):
        return {
            RING[k]: lax.rem(index[k] + size[k] + (-step if back else step), size[k])
            for k, step in enumerate(offset)
            if step
        }

    barrier = pltpu.get_barrier_semaphore()

    def greet(offset):
        pl.semaphore_signal(barrier, inc=1, device_id=device(offset, back=True), device_id_type=MESH)

    fetch = [
        pltpu.make_async_copy(links_ref.at[pl.ds(mu * 18, 18)], u.at[pl.ds(mu * 18, 18)], in_sem.at[mu])
        for mu in range(4)
    ]
    for copy in fetch:
        copy.start()

    for offset in OUTGOING:
        if offset not in WRAP_LATER:
            greet(offset)

    @pl.when(jnp.logical_not(last_time))
    def _():
        for offset in WRAP_LATER:
            greet(offset)

    @pl.when(first_time)
    def _():
        for offset in WRAP_SOONER:
            greet(offset)

    for copy in fetch:
        copy.wait()

    def link(mu, part, i, j):
        return lambda: u[comp(mu, part, i, j)]

    for d in FACES:
        pack([link(nu, *c) for c in TWO_ROWS for nu in others(d) + [d]], send2[d], d, high=True)
    for number, (d, e) in enumerate(EDGES):
        pack_edge([link(d, *c) for c in TWO_ROWS], sende[number], d, e)
    for d in (1, 0, 2):
        pack([link(nu, *c) for nu in others(d) for c in TWO_ROWS], send1[d], d, high=False)

    @pl.when(first_time)
    def _():
        pl.semaphore_wait(barrier, len(OUTGOING) - len(WRAP_LATER))

    @pl.when(last_time)
    def _():
        pl.semaphore_wait(barrier, len(OUTGOING) + len(WRAP_SOONER))

    @pl.when(jnp.logical_not(first_time | last_time))
    def _():
        pl.semaphore_wait(barrier, len(OUTGOING))

    def remote(src, dst, send, recv, offset):
        return pltpu.make_async_remote_copy(
            src_ref=src, dst_ref=dst, send_sem=send, recv_sem=recv,
            device_id=device(offset), device_id_type=MESH,
        )

    down = [remote(send1[d], recv1[d], s1.at[d], r1.at[d], DOWN[d]) for d in range(3)]
    up = [remote(send2[d], recv2[d], s2.at[d], r2.at[d], UP[d]) for d in range(3)]
    corner = {
        pair: remote(sende[n], recve[n], se.at[n], re.at[n], CORNER[n]) for n, pair in enumerate(EDGES)
    }
    down[2].start()
    up[0].start()
    down[0].start()
    up[1].start()
    down[1].start()
    up[2].start()
    corner[1, 2].start()

    def start_up_time():
        corner[0, 1].start()
        corner[0, 2].start()

    pl.when(last_time)(start_up_time)

    @pl.when(jnp.logical_not(first_time))
    def _():
        corner[1, 0].start()
        corner[2, 0].start()

    def make_w(plane, mu, nu):
        def body(v, carry):
            rows = pl.ds(pl.multiple_of(v * 8, 8), 8)

            def get(ref, base):
                return [[(ref[base + i * 3 + j, rows, :], ref[base + 9 + i * 3 + j, rows, :])
                         for j in range(3)] for i in range(3)]

            a = get(u, mu * 18)
            b = get(u, nu * 18)
            for i in range(3):
                for j in range(3):
                    real, imag = dot3([(b[k][i], a[k][j]) for k in range(3)], conj_a=True)
                    wmat[plane * 18 + i * 3 + j, rows, :] = real
                    wmat[plane * 18 + 9 + i * 3 + j, rows, :] = imag
            return carry

        lax.fori_loop(0, 2, body, 0)

    def shift_x():
        for nu in others(3):
            at = slot(3, nu) * 18
            for c in range(18):
                shifted[at + c] = shift_within_x(u[nu * 18 + c])

    def shift_split(d):
        edge = position(d) == COUNT[d] - 1
        for order, nu in enumerate(others(d)):
            at = slot(d, nu) * 18
            got = {}
            for number, (part, i, j) in enumerate(TWO_ROWS):
                local = turn(u[comp(nu, part, i, j)], d, -1)
                value = jnp.where(edge, unpack(recv1[d], order * 12 + number, d, high=True), local)
                got[part, i, j] = value
                shifted[at + part * 9 + i * 3 + j] = value

            def put(part, j, value, at=at):
                shifted[at + part * 9 + 6 + j] = value

            third_row(lambda *c: got[c], put)

    def face_near(d):
        where = position(d)
        for c in range(18):
            value = None
            for j, nu in enumerate(others(d)):
                part = turn(u[nu * 18 + c], d, j)
                value = part if value is None else jnp.where(where == j, part, value)
            near[d * 18 + c] = value

    def face_leaf(d):
        where = position(d)
        got_far, got_base, got_moved = {}, {}, {}
        per_tile = GROUP[d] // 4
        for number, c in enumerate(TWO_ROWS):
            value = turn(recv2[d][number // per_tile], d, -4 * (number % per_tile))
            got_far[c] = value
            spread = value
            for j in range(3):
                spread = jnp.where(where == j, turn(value, d, j - 3), spread)
            got_base[c] = spread
            shift = shift_within_x(spread)
            for j, mu in enumerate(others(d)):
                if mu == 3:
                    continue
                edge = EDGES.index((d, mu))
                step = jnp.where(
                    position(mu) == COUNT[mu] - 1,
                    unpack_edge(recve[edge], d, mu, number, j),
                    turn(spread, mu, -1),
                )
                shift = jnp.where(where == j, step, shift)
            got_moved[c] = shift
        for ref, got in ((far, got_far), (base, got_base), (moved, got_moved)):
            for (part, i, j), value in got.items():
                ref[part * 9 + i * 3 + j] = value

            def put(part, j, value, ref=ref):
                ref[part * 9 + 6 + j] = value

            third_row(lambda *c: got[c], put)

        def body(v, carry):
            rows = pl.ds(pl.multiple_of(v * 8, 8), 8)

            def get(ref, at, i, j):
                return (ref[at + i * 3 + j, rows, :], ref[at + 9 + i * 3 + j, rows, :])

            g = [[None] * 3 for _ in range(3)]
            for i in range(3):
                hi = [get(far, 0, i, k) for k in range(3)]
                for j in range(3):
                    g[i][j] = dot3([(hi[k], get(moved, 0, k, j)) for k in range(3)])
            x = [[None] * 3 for _ in range(3)]
            for i in range(3):
                ai = [get(near, d * 18, i, k) for k in range(3)]
                for j in range(3):
                    x[i][j] = dot3([(ai[k], g[j][k]) for k in range(3)], conj_b=True)

            def entry(i, j, parts):
                return dot3([(x[i][k], get(base, 0, k, j)) for k in range(3)], parts=parts)

            diag = [entry(i, i, "i")[1] for i in range(3)]
            trace = (diag[0] + diag[1] + diag[2]) * (1.0 / 3.0)
            values = leaf(lambda i, j, parts: (None, diag[i]) if i == j else entry(i, j, parts), trace)
            for c in range(8):
                faceleaf[c, rows, :] = values[c]
            return carry

        lax.fori_loop(0, 2, body, 0)

    seen = set()

    def do_plane(plane, mu, nu):
        fresh_mu, fresh_nu = mu not in seen, nu not in seen
        seen.update((mu, nu))

        def body(v, carry):
            rows = pl.ds(pl.multiple_of(v * 8, 8), 8)

            def get(ref, base, i, j):
                return (ref[base + i * 3 + j, rows, :], ref[base + 9 + i * 3 + j, rows, :])

            cbase = slot(mu, nu) * 18
            dbase = slot(nu, mu) * 18
            t = [[None] * 3 for _ in range(3)]
            for i in range(3):
                ci = [get(shifted, cbase, i, k) for k in range(3)]
                for j in range(3):
                    t[i][j] = dot3([(ci[k], get(shifted, dbase, j, k)) for k in range(3)], conj_b=True)

            x = [[None] * 3 for _ in range(3)]
            for i in range(3):
                ai = [get(u, mu * 18, i, k) for k in range(3)]
                for j in range(3):
                    x[i][j] = dot3([(ai[k], t[k][j]) for k in range(3)])

            def p_entry(i, j, parts):
                return dot3([(x[i][k], get(u, nu * 18, j, k)) for k in range(3)], conj_b=True, parts=parts)

            diag = [p_entry(i, i, "i")[1] for i in range(3)]
            trace = (diag[0] + diag[1] + diag[2]) * (1.0 / 3.0)
            values = leaf(lambda i, j, parts: (None, diag[i]) if i == j else p_entry(i, j, parts), trace)
            for c in range(8):
                at_mu = (mu * 8 + c, rows, slice(None))
                at_nu = (nu * 8 + c, rows, slice(None))
                if fresh_mu:
                    store[at_mu] = values[c]
                else:
                    store[at_mu] = store[at_mu] + values[c]
                if fresh_nu:
                    store[at_nu] = -values[c]
                else:
                    store[at_nu] = store[at_nu] - values[c]

            def w(i, j):
                return get(wmat, plane * 18, i, j)

            values = leaf(lambda i, j, parts: dot3([(w(i, k), t[k][j]) for k in range(3)], parts=parts), trace)
            for c in range(8):
                leaves[slot(nu, mu) * 8 + c, rows, :] = values[c]
            values = leaf(lambda i, j, parts: dot3([(t[i][k], w(k, j)) for k in range(3)], parts=parts), trace)
            for c in range(8):
                leaves[slot(mu, nu) * 8 + c, rows, :] = values[c]
            return carry

        lax.fori_loop(0, 2, body, 0)

    shift_x()
    for plane, (mu, nu) in enumerate(PLANES):
        make_w(plane, mu, nu)
    for d in FACES:
        face_near(d)
    down[2].wait_recv()
    corner[2, 1].start()
    pl.when(first_time)(corner[2, 0].start)
    shift_split(2)
    do_plane(1, 2, 3)
    down[0].wait_recv()
    pl.when(jnp.logical_not(last_time))(start_up_time)
    shift_split(0)
    do_plane(0, 0, 3)
    do_plane(2, 0, 2)
    down[1].wait_recv()
    pl.when(first_time)(corner[1, 0].start)
    shift_split(1)
    do_plane(3, 1, 3)
    do_plane(4, 1, 2)
    do_plane(5, 0, 1)

    def sign(d, nu):
        return -1 if (nu, d) in PLANES else 1

    for nu in range(4):
        for c in range(8):
            value = store[nu * 8 + c]
            for d in others(nu):
                moved_leaf = leaves[slot(d, nu) * 8 + c]
                first = position(d) == 0
                if d == 3:
                    around = pltpu.roll(moved_leaf, LANES - NX + 1, axis=1)
                    moved_leaf = jnp.where(first, around, pltpu.roll(moved_leaf, 1, axis=1))
                else:
                    moved_leaf = jnp.where(first, 0.0, turn(moved_leaf, d, 1))
                value = value + moved_leaf if sign(d, nu) > 0 else value - moved_leaf
            store[nu * 8 + c] = value

    for d in (2, 1, 0):
        up[d].wait_recv()
        for pair in EDGES:
            if pair[0] == d:
                corner[pair].wait_recv()
        face_leaf(d)
        first = position(d) == 0
        for order, nu in enumerate(others(d)):
            for c in range(8):
                store[nu * 8 + c] += jnp.where(first, turn(faceleaf[c], d, -order), 0.0)

    for mu in range(4):
        for number, (i, j) in enumerate(OFF):
            real = store[mu * 8 + number * 2] * (0.5 * COEFF)
            imag = store[mu * 8 + number * 2 + 1] * (0.5 * COEFF)
            out_ref[comp(mu, 0, i, j)] = real
            out_ref[comp(mu, 0, j, i)] = -real
            out_ref[comp(mu, 1, i, j)] = imag
            out_ref[comp(mu, 1, j, i)] = imag
        diag0 = store[mu * 8 + 6] * COEFF
        diag1 = store[mu * 8 + 7] * COEFF
        for i, value in enumerate((diag0, diag1, -(diag0 + diag1))):
            out_ref[comp(mu, 1, i, i)] = value
            out_ref[comp(mu, 0, i, i)] = jnp.zeros_like(value)

    for copy in down + up + list(corner.values()):
        copy.wait_send()


def per_device(links):
    shape = links.shape
    vmem = pltpu.VMEM

    def packed(counts):
        return [vmem((n, ROWS, LANES), jnp.float32) for n in counts]

    counts1 = [-(-36 // g) for g in GROUP]
    counts2 = (12, 12, 6)
    edges = [vmem((ROWS, LANES), jnp.float32) for _ in EDGES]
    arrays = (72, 216, 32, 96, 108)
    dma = pltpu.SemaphoreType.DMA
    out = pl.pallas_call(
        kernel,
        out_shape=jax.ShapeDtypeStruct((72, ROWS, LANES), jnp.float32),
        in_specs=[pl.BlockSpec(memory_space=pltpu.HBM)],
        out_specs=pl.BlockSpec(memory_space=pltpu.VMEM),
        scratch_shapes=packed(arrays)
        + [packed(counts1), packed(counts1), packed(counts2), packed(counts2), edges, edges]
        + packed((54, 18, 18, 18, 8))
        + [dma((n,)) for n in (4, 3, 3, 3, 3, 6, 6)],
        compiler_params=pltpu.CompilerParams(
            collective_id=0, has_side_effects=True, vmem_limit_bytes=16 * 1024 * 1024
        ),
    )(pltpu.with_memory_space_constraint(links.reshape(72, ROWS, LANES), pltpu.HBM))
    return out.reshape(shape)


def solution(mesh):
    return jax.shard_map(
        per_device,
        mesh=mesh,
        in_specs=(P(None, None, None, None, "ta", "gz", "gx"),),
        out_specs=P(None, None, None, None, "ta", "gz", "gx"),
        check_vma=False,
    )
```

```python
import functools

import jax
import jax.numpy as jnp
from jax import lax
from jax.experimental import pallas as pl
from jax.experimental.pallas import tpu as pltpu
from jax.sharding import PartitionSpec as P

MESH = pl.DeviceIdType.MESH
COEFF = -1.9
NX = 16
ROWS = 16
LANES = 128

STEP = (4, 1, 16, 1)
AXIS = (0, 0, 1, 1)
COUNT = (4, 4, 8, 16)
GROUP = (4, 4, 8)
RING = ("ta", "gz", "gx")
PLANES = ((0, 3), (2, 3), (0, 2), (1, 3), (1, 2), (0, 1))


def comp(mu, part, i, j):
    return ((mu * 2 + part) * 3 + i) * 3 + j


def slot(step_dir, link_dir):
    return step_dir * 3 + (link_dir if link_dir < step_dir else link_dir - 1)


def others(direction):
    return [d for d in range(4) if d != direction]


def position(direction):
    iota = lax.broadcasted_iota(jnp.int32, (ROWS, LANES), AXIS[direction])
    return (iota // STEP[direction]) % COUNT[direction]


def turn(value, direction, steps):
    size = (ROWS, LANES)[AXIS[direction]]
    amount = (steps * STEP[direction]) % size
    if amount == 0:
        return value
    return pltpu.roll(value, amount, axis=AXIS[direction])


def pack(loads, buf, direction, high):
    where = position(direction)
    width = GROUP[direction]
    for first in range(0, len(loads), width):
        packed = None
        for j, load in enumerate(loads[first : first + width]):
            moved = turn(load(), direction, j - (width - 1) if high else j)
            packed = moved if packed is None else jnp.where(where == j, moved, packed)
        buf[first // width] = packed


def unpack(buf, index, direction, high):
    width = GROUP[direction]
    j = index % width
    return turn(buf[index // width], direction, width - 1 - j if high else -j)


def edge_place(d, e, c):
    return (c // 8, c % 8) if e == 2 else (c % 4, c // 4)


def pack_edge(loads, buf, d, e):
    packed = None
    for c, load in enumerate(loads):
        at_d, at_e = edge_place(d, e, c)
        moved = turn(turn(load(), d, at_d - (COUNT[d] - 1)), e, at_e)
        here = (position(d) == at_d) & (position(e) == at_e)
        packed = moved if packed is None else jnp.where(here, moved, packed)
    buf[...] = packed


def unpack_edge(buf, d, e, c, to_d):
    at_d, at_e = edge_place(d, e, c)
    return turn(turn(buf[...], d, to_d - at_d), e, COUNT[e] - 1 - at_e)


def shift_within_x(value):
    edge = position(3) == NX - 1
    return jnp.where(edge, pltpu.roll(value, NX - 1, axis=1), pltpu.roll(value, LANES - 1, axis=1))


def third_row(get, put):
    for j in range(3):
        p, q = (j + 1) % 3, (j + 2) % 3
        r0p, r0q, r1p, r1q = get(0, 0, p), get(0, 0, q), get(0, 1, p), get(0, 1, q)
        i0p, i0q, i1p, i1q = get(1, 0, p), get(1, 0, q), get(1, 1, p), get(1, 1, q)
        put(0, j, r0p * r1q - i0p * i1q - r0q * r1p + i0q * i1p)
        put(1, j, r0q * i1p + i0q * r1p - r0p * i1q - i0p * r1q)


def total(terms):
    terms = sorted(terms, key=lambda term: -term[0])
    result = None
    for sign, value in terms:
        if result is None:
            result = value if sign > 0 else -value
        else:
            result = result + value if sign > 0 else result - value
    return result


def dot3(pairs, conj_a=False, conj_b=False, parts="ri"):
    real, imag = [], []
    for a, b in pairs:
        (ar, ai), (br, bi) = a, b
        sa = -1 if conj_a else 1
        sb = -1 if conj_b else 1
        if "r" in parts:
            real += [(1, ar * br), (-sa * sb, ai * bi)]
        if "i" in parts:
            imag += [(sb, ar * bi), (sa, ai * br)]
    return (total(real) if real else None, total(imag) if imag else None)


OFF = ((0, 1), (0, 2), (1, 2))


def leaf(entry, trace):
    values = []
    for i, j in OFF:
        upper = entry(i, j, "ri")
        lower = entry(j, i, "ri")
        values.append(upper[0] - lower[0])
        values.append(upper[1] + lower[1])
    for i in range(2):
        values.append(entry(i, i, "i")[1] - trace)
    return values


FACES = (0, 1, 2)
EDGES = ((0, 1), (0, 2), (1, 0), (1, 2), (2, 0), (2, 1))


def offset_of(plus=None, minus=None):
    return tuple(1 if k == plus else -1 if k == minus else 0 for k in range(3))


DOWN = [offset_of(minus=d) for d in range(3)]
UP = [offset_of(plus=d) for d in range(3)]
CORNER = [offset_of(d, e) for d, e in EDGES]
CORNER_AT = dict(zip(EDGES, CORNER))
TWO_ROWS = [(part, i, j) for part in range(2) for i in range(2) for j in range(3)]


def kernel(links_ref, out_ref, u, shifted, store, leaves, wmat, send1, recv1, send2, recv2, sende, recve,
           near, far, base, moved, faceleaf, in_sem, s1, r1, s2, r2, se, re):
    index = [lax.axis_index(name) for name in RING]
    size = [lax.axis_size(name) for name in RING]
    first_time = index[0] == 0
    last_time = index[0] == size[0] - 1
    first_z = index[1] == 0
    last_z = index[1] == size[1] - 1

    def no(condition):
        return jnp.logical_not(condition)

    def device(offset, back=False):
        return {
            RING[k]: lax.rem(index[k] + size[k] + (-step if back else step), size[k])
            for k, step in enumerate(offset)
            if step
        }

    barrier = pltpu.get_barrier_semaphore()

    def greet(offset):
        pl.semaphore_signal(barrier, inc=1, device_id=device(offset, back=True), device_id_type=MESH)

    fetch = [
        pltpu.make_async_copy(links_ref.at[pl.ds(mu * 18, 18)], u.at[pl.ds(mu * 18, 18)], in_sem.at[mu])
        for mu in range(4)
    ]
    for copy in fetch:
        copy.start()

    for offset in (DOWN[2], UP[2], CORNER_AT[1, 2]):
        greet(offset)
    pl.when(no(first_time))(lambda: greet(UP[0]))
    pl.when(no(first_z))(lambda: greet(UP[1]))
    pl.when(no(last_z))(lambda: greet(DOWN[1]))

    @pl.when(no(last_time))
    def _():
        for offset in (DOWN[0], CORNER_AT[1, 0], CORNER_AT[2, 0]):
            greet(offset)

    @pl.when(first_time)
    def _():
        for offset in (CORNER_AT[0, 1], CORNER_AT[0, 2]):
            greet(offset)

    for copy in fetch:
        copy.wait()

    def link(mu, part, i, j):
        return lambda: u[comp(mu, part, i, j)]

    for d in FACES:
        pack([link(nu, *c) for c in TWO_ROWS for nu in others(d) + [d]], send2[d], d, high=True)
    for number, (d, e) in enumerate(EDGES):
        pack_edge([link(d, *c) for c in TWO_ROWS], sende[number], d, e)
    for d in (1, 0, 2):
        pack([link(nu, *c) for nu in others(d) for c in TWO_ROWS], send1[d], d, high=False)

    middle = no(first_time | last_time)
    for here, count in ((first_time, 6), (middle, 9), (last_time, 11)):
        pl.when(here & first_z)(functools.partial(pl.semaphore_wait, barrier, count - 1))
        pl.when(here & no(first_z))(functools.partial(pl.semaphore_wait, barrier, count))
    pl.when(first_time)(lambda: greet(UP[0]))
    pl.when(first_z)(lambda: greet(UP[1]))
    pl.when(last_time)(lambda: greet(DOWN[0]))
    pl.when(last_z)(lambda: greet(DOWN[1]))

    def remote(src, dst, send, recv, offset):
        return pltpu.make_async_remote_copy(
            src_ref=src, dst_ref=dst, send_sem=send, recv_sem=recv,
            device_id=device(offset), device_id_type=MESH,
        )

    down = [remote(send1[d], recv1[d], s1.at[d], r1.at[d], DOWN[d]) for d in range(3)]
    up = [remote(send2[d], recv2[d], s2.at[d], r2.at[d], UP[d]) for d in range(3)]
    corner = {
        pair: remote(sende[n], recve[n], se.at[n], re.at[n], CORNER[n]) for n, pair in enumerate(EDGES)
    }
    def start(*copies):
        def body():
            for copy in copies:
                copy.start()

        return body

    corner[1, 2].start()
    pl.when(last_time)(start(corner[0, 1], corner[0, 2]))
    pl.when(no(first_time))(start(corner[1, 0], corner[2, 0]))
    down[2].start()
    up[0].start()
    pl.when(no(first_time))(down[0].start)
    up[1].start()
    pl.when(no(first_z))(down[1].start)
    up[2].start()

    def second_stage():
        pl.when(first_time & first_z)(lambda: pl.semaphore_wait(barrier, 2))
        pl.when(first_time & no(first_z))(lambda: pl.semaphore_wait(barrier, 1))
        pl.when(no(first_time) & first_z)(lambda: pl.semaphore_wait(barrier, 1))
        pl.when(first_z)(corner[2, 1].start)
        pl.when(first_z & no(last_time))(corner[0, 1].start)
        pl.when(first_z)(down[1].start)
        pl.when(first_time)(start(corner[1, 0], corner[2, 0], down[0]))

    def make_w(plane, mu, nu):
        def body(v, carry):
            rows = pl.ds(pl.multiple_of(v * 8, 8), 8)

            def get(ref, base):
                return [[(ref[base + i * 3 + j, rows, :], ref[base + 9 + i * 3 + j, rows, :])
                         for j in range(3)] for i in range(3)]

            a = get(u, mu * 18)
            b = get(u, nu * 18)
            for i in range(3):
                for j in range(3):
                    real, imag = dot3([(b[k][i], a[k][j]) for k in range(3)], conj_a=True)
                    wmat[plane * 18 + i * 3 + j, rows, :] = real
                    wmat[plane * 18 + 9 + i * 3 + j, rows, :] = imag
            return carry

        lax.fori_loop(0, 2, body, 0)

    def shift_x():
        for nu in others(3):
            at = slot(3, nu) * 18
            for c in range(18):
                shifted[at + c] = shift_within_x(u[nu * 18 + c])

    def shift_split(d):
        edge = position(d) == COUNT[d] - 1
        for order, nu in enumerate(others(d)):
            at = slot(d, nu) * 18
            got = {}
            for number, (part, i, j) in enumerate(TWO_ROWS):
                local = turn(u[comp(nu, part, i, j)], d, -1)
                value = jnp.where(edge, unpack(recv1[d], order * 12 + number, d, high=True), local)
                got[part, i, j] = value
                shifted[at + part * 9 + i * 3 + j] = value

            def put(part, j, value, at=at):
                shifted[at + part * 9 + 6 + j] = value

            third_row(lambda *c: got[c], put)

    def face_near(d):
        where = position(d)
        for c in range(18):
            value = None
            for j, nu in enumerate(others(d)):
                part = turn(u[nu * 18 + c], d, j)
                value = part if value is None else jnp.where(where == j, part, value)
            near[d * 18 + c] = value

    def face_leaf(d):
        where = position(d)
        got_far, got_base, got_moved = {}, {}, {}
        per_tile = GROUP[d] // 4
        for number, c in enumerate(TWO_ROWS):
            value = turn(recv2[d][number // per_tile], d, -4 * (number % per_tile))
            got_far[c] = value
            spread = value
            for j in range(3):
                spread = jnp.where(where == j, turn(value, d, j - 3), spread)
            got_base[c] = spread
            shift = shift_within_x(spread)
            for j, mu in enumerate(others(d)):
                if mu == 3:
                    continue
                edge = EDGES.index((d, mu))
                step = jnp.where(
                    position(mu) == COUNT[mu] - 1,
                    unpack_edge(recve[edge], d, mu, number, j),
                    turn(spread, mu, -1),
                )
                shift = jnp.where(where == j, step, shift)
            got_moved[c] = shift
        for ref, got in ((far, got_far), (base, got_base), (moved, got_moved)):
            for (part, i, j), value in got.items():
                ref[part * 9 + i * 3 + j] = value

            def put(part, j, value, ref=ref):
                ref[part * 9 + 6 + j] = value

            third_row(lambda *c: got[c], put)

        def body(v, carry):
            rows = pl.ds(pl.multiple_of(v * 8, 8), 8)

            def get(ref, at, i, j):
                return (ref[at + i * 3 + j, rows, :], ref[at + 9 + i * 3 + j, rows, :])

            g = [[None] * 3 for _ in range(3)]
            for i in range(3):
                hi = [get(far, 0, i, k) for k in range(3)]
                for j in range(3):
                    g[i][j] = dot3([(hi[k], get(moved, 0, k, j)) for k in range(3)])
            x = [[None] * 3 for _ in range(3)]
            for i in range(3):
                ai = [get(near, d * 18, i, k) for k in range(3)]
                for j in range(3):
                    x[i][j] = dot3([(ai[k], g[j][k]) for k in range(3)], conj_b=True)

            def entry(i, j, parts):
                return dot3([(x[i][k], get(base, 0, k, j)) for k in range(3)], parts=parts)

            diag = [entry(i, i, "i")[1] for i in range(3)]
            trace = (diag[0] + diag[1] + diag[2]) * (1.0 / 3.0)
            values = leaf(lambda i, j, parts: (None, diag[i]) if i == j else entry(i, j, parts), trace)
            for c in range(8):
                faceleaf[c, rows, :] = values[c]
            return carry

        lax.fori_loop(0, 2, body, 0)

    def do_plane(plane, mu, nu):
        def body(v, carry):
            rows = pl.ds(pl.multiple_of(v * 8, 8), 8)

            def get(ref, base, i, j):
                return (ref[base + i * 3 + j, rows, :], ref[base + 9 + i * 3 + j, rows, :])

            cbase = slot(mu, nu) * 18
            dbase = slot(nu, mu) * 18
            t = [[None] * 3 for _ in range(3)]
            for i in range(3):
                ci = [get(shifted, cbase, i, k) for k in range(3)]
                for j in range(3):
                    t[i][j] = dot3([(ci[k], get(shifted, dbase, j, k)) for k in range(3)], conj_b=True)

            x = [[None] * 3 for _ in range(3)]
            for i in range(3):
                ai = [get(u, mu * 18, i, k) for k in range(3)]
                for j in range(3):
                    x[i][j] = dot3([(ai[k], t[k][j]) for k in range(3)])

            def p_entry(i, j, parts):
                return dot3([(x[i][k], get(u, nu * 18, j, k)) for k in range(3)], conj_b=True, parts=parts)

            diag = [p_entry(i, i, "i")[1] for i in range(3)]
            trace = (diag[0] + diag[1] + diag[2]) * (1.0 / 3.0)
            values = leaf(lambda i, j, parts: (None, diag[i]) if i == j else p_entry(i, j, parts), trace)
            for c in range(8):
                at_mu = (mu * 8 + c, rows, slice(None))
                at_nu = (nu * 8 + c, rows, slice(None))
                store[at_mu] = store[at_mu] + values[c]
                store[at_nu] = store[at_nu] - values[c]

            def w(i, j):
                return get(wmat, plane * 18, i, j)

            values = leaf(lambda i, j, parts: dot3([(w(i, k), t[k][j]) for k in range(3)], parts=parts), trace)
            for c in range(8):
                leaves[slot(nu, mu) * 8 + c, rows, :] = values[c]
            values = leaf(lambda i, j, parts: dot3([(t[i][k], w(k, j)) for k in range(3)], parts=parts), trace)
            for c in range(8):
                leaves[slot(mu, nu) * 8 + c, rows, :] = values[c]
            return carry

        lax.fori_loop(0, 2, body, 0)

    store[...] = jnp.zeros_like(store)
    shift_x()
    for plane, (mu, nu) in enumerate(PLANES):
        make_w(plane, mu, nu)
    for d in FACES:
        face_near(d)
    down[2].wait_recv()
    pl.when(no(first_z))(corner[2, 1].start)
    shift_split(2)
    do_plane(1, 2, 3)
    down[0].wait_recv()
    pl.when(no(last_time))(corner[0, 2].start)
    pl.when(no(last_time | first_z))(corner[0, 1].start)
    shift_split(0)
    do_plane(0, 0, 3)
    do_plane(2, 0, 2)

    def planes_z():
        down[1].wait_recv()
        shift_split(1)
        do_plane(3, 1, 3)
        do_plane(4, 1, 2)
        do_plane(5, 0, 1)

    def face(d):
        up[d].wait_recv()
        for pair in EDGES:
            if pair[0] == d:
                corner[pair].wait_recv()
        face_leaf(d)
        first = position(d) == 0
        for order, nu in enumerate(others(d)):
            for c in range(8):
                store[nu * 8 + c] += jnp.where(first, turn(faceleaf[c], d, -order), 0.0)

    second_stage()
    stages = (planes_z, functools.partial(face, 2), functools.partial(face, 0), functools.partial(face, 1))
    orders = (
        (no(first_time | last_z), (0, 1, 2, 3)),
        (first_time & no(last_z), (0, 1, 3, 2)),
        (last_z & no(first_time), (3, 2, 1, 0)),
        (first_time & last_z, (3, 1, 0, 2)),
    )

    def take(step, carry):
        for number, stage in enumerate(stages):
            now = None
            for here, order in orders:
                hit = here & (step == order.index(number))
                now = hit if now is None else now | hit
            pl.when(now)(stage)
        return carry

    lax.fori_loop(0, len(stages), take, 0)

    def sign(d, nu):
        return -1 if (nu, d) in PLANES else 1

    def final(nu, c):
        value = store[nu * 8 + c]
        for d in others(nu):
            moved_leaf = leaves[slot(d, nu) * 8 + c]
            first = position(d) == 0
            if d == 3:
                around = pltpu.roll(moved_leaf, LANES - NX + 1, axis=1)
                moved_leaf = jnp.where(first, around, pltpu.roll(moved_leaf, 1, axis=1))
            else:
                moved_leaf = jnp.where(first, 0.0, turn(moved_leaf, d, 1))
            value = value + moved_leaf if sign(d, nu) > 0 else value - moved_leaf
        return value

    for mu in range(4):
        for number, (i, j) in enumerate(OFF):
            real = final(mu, number * 2) * (0.5 * COEFF)
            imag = final(mu, number * 2 + 1) * (0.5 * COEFF)
            out_ref[comp(mu, 0, i, j)] = real
            out_ref[comp(mu, 0, j, i)] = -real
            out_ref[comp(mu, 1, i, j)] = imag
            out_ref[comp(mu, 1, j, i)] = imag
        diag0 = final(mu, 6) * COEFF
        diag1 = final(mu, 7) * COEFF
        for i, value in enumerate((diag0, diag1, -(diag0 + diag1))):
            out_ref[comp(mu, 1, i, i)] = value
            out_ref[comp(mu, 0, i, i)] = jnp.zeros_like(value)

    for copy in down + up + list(corner.values()):
        copy.wait_send()


def per_device(links):
    shape = links.shape
    vmem = pltpu.VMEM

    def packed(counts):
        return [vmem((n, ROWS, LANES), jnp.float32) for n in counts]

    counts1 = [-(-36 // g) for g in GROUP]
    counts2 = (12, 12, 6)
    edges = [vmem((ROWS, LANES), jnp.float32) for _ in EDGES]
    arrays = (72, 216, 32, 96, 108)
    dma = pltpu.SemaphoreType.DMA
    out = pl.pallas_call(
        kernel,
        out_shape=jax.ShapeDtypeStruct((72, ROWS, LANES), jnp.float32),
        in_specs=[pl.BlockSpec(memory_space=pltpu.HBM)],
        out_specs=pl.BlockSpec(memory_space=pltpu.VMEM),
        scratch_shapes=packed(arrays)
        + [packed(counts1), packed(counts1), packed(counts2), packed(counts2), edges, edges]
        + packed((54, 18, 18, 18, 8))
        + [dma((n,)) for n in (4, 3, 3, 3, 3, 6, 6)],
        compiler_params=pltpu.CompilerParams(
            collective_id=0, has_side_effects=True, vmem_limit_bytes=16 * 1024 * 1024
        ),
    )(pltpu.with_memory_space_constraint(links.reshape(72, ROWS, LANES), pltpu.HBM))
    return out.reshape(shape)


def solution(mesh):
    return jax.shard_map(
        per_device,
        mesh=mesh,
        in_specs=(P(None, None, None, None, "ta", "gz", "gx"),),
        out_specs=P(None, None, None, None, "ta", "gz", "gx"),
        check_vma=False,
    )
```

```python
import functools

import jax
import jax.numpy as jnp
from jax import lax
from jax.experimental import pallas as pl
from jax.experimental.pallas import tpu as pltpu
from jax.sharding import PartitionSpec as P

MESH = pl.DeviceIdType.MESH
COEFF = -1.9
NX = 16
ROWS = 16
LANES = 128

STEP = (4, 1, 16, 1)
AXIS = (0, 0, 1, 1)
COUNT = (4, 4, 8, 16)
GROUP = (4, 4, 8)
RING = ("ta", "gz", "gx")
PLANES = ((0, 3), (2, 3), (0, 2), (1, 3), (1, 2), (0, 1))


def comp(mu, part, i, j):
    return ((mu * 2 + part) * 3 + i) * 3 + j


def slot(step_dir, link_dir):
    return step_dir * 3 + (link_dir if link_dir < step_dir else link_dir - 1)


def others(direction):
    return [d for d in range(4) if d != direction]


def position(direction):
    iota = lax.broadcasted_iota(jnp.int32, (ROWS, LANES), AXIS[direction])
    return (iota // STEP[direction]) % COUNT[direction]


def turn(value, direction, steps):
    size = (ROWS, LANES)[AXIS[direction]]
    amount = (steps * STEP[direction]) % size
    if amount == 0:
        return value
    return pltpu.roll(value, amount, axis=AXIS[direction])


def pack(loads, buf, direction, high):
    where = position(direction)
    width = GROUP[direction]
    for first in range(0, len(loads), width):
        packed = None
        for j, load in enumerate(loads[first : first + width]):
            moved = turn(load(), direction, j - (width - 1) if high else j)
            packed = moved if packed is None else jnp.where(where == j, moved, packed)
        buf[first // width] = packed


def unpack(buf, index, direction, high):
    width = GROUP[direction]
    j = index % width
    return turn(buf[index // width], direction, width - 1 - j if high else -j)


def edge_place(d, e, c):
    return (c // 8, c % 8) if e == 2 else (c % 4, c // 4)


def pack_edge(loads, buf, d, e):
    packed = None
    for c, load in enumerate(loads):
        at_d, at_e = edge_place(d, e, c)
        moved = turn(turn(load(), d, at_d - (COUNT[d] - 1)), e, at_e)
        here = (position(d) == at_d) & (position(e) == at_e)
        packed = moved if packed is None else jnp.where(here, moved, packed)
    buf[...] = packed


def unpack_edge(buf, d, e, c, to_d):
    at_d, at_e = edge_place(d, e, c)
    return turn(turn(buf[...], d, to_d - at_d), e, COUNT[e] - 1 - at_e)


def shift_within_x(value):
    edge = position(3) == NX - 1
    return jnp.where(edge, pltpu.roll(value, NX - 1, axis=1), pltpu.roll(value, LANES - 1, axis=1))


def third_row(get, put):
    for j in range(3):
        p, q = (j + 1) % 3, (j + 2) % 3
        r0p, r0q, r1p, r1q = get(0, 0, p), get(0, 0, q), get(0, 1, p), get(0, 1, q)
        i0p, i0q, i1p, i1q = get(1, 0, p), get(1, 0, q), get(1, 1, p), get(1, 1, q)
        put(0, j, r0p * r1q - i0p * i1q - r0q * r1p + i0q * i1p)
        put(1, j, r0q * i1p + i0q * r1p - r0p * i1q - i0p * r1q)


def total(terms):
    terms = sorted(terms, key=lambda term: -term[0])
    result = None
    for sign, value in terms:
        if result is None:
            result = value if sign > 0 else -value
        else:
            result = result + value if sign > 0 else result - value
    return result


def dot3(pairs, conj_a=False, conj_b=False, parts="ri"):
    real, imag = [], []
    for a, b in pairs:
        (ar, ai), (br, bi) = a, b
        sa = -1 if conj_a else 1
        sb = -1 if conj_b else 1
        if "r" in parts:
            real += [(1, ar * br), (-sa * sb, ai * bi)]
        if "i" in parts:
            imag += [(sb, ar * bi), (sa, ai * br)]
    return (total(real) if real else None, total(imag) if imag else None)


OFF = ((0, 1), (0, 2), (1, 2))


def leaf(entry, trace):
    values = []
    for i, j in OFF:
        upper = entry(i, j, "ri")
        lower = entry(j, i, "ri")
        values.append(upper[0] - lower[0])
        values.append(upper[1] + lower[1])
    for i in range(2):
        values.append(entry(i, i, "i")[1] - trace)
    return values


FACES = (0, 1, 2)
EDGES = ((0, 1), (0, 2), (1, 0), (1, 2), (2, 0), (2, 1))


def offset_of(plus=None, minus=None):
    return tuple(1 if k == plus else -1 if k == minus else 0 for k in range(3))


DOWN = [offset_of(minus=d) for d in range(3)]
UP = [offset_of(plus=d) for d in range(3)]
CORNER = [offset_of(d, e) for d, e in EDGES]
CORNER_AT = dict(zip(EDGES, CORNER))
TWO_ROWS = [(part, i, j) for part in range(2) for i in range(2) for j in range(3)]


def kernel(links_ref, store, leaves, u, shifted, wmat, send1, recv1, send2, recv2, sende, recve,
           near, far, base, moved, faceleaf, in_sem, s1, r1, s2, r2, se, re, sz, rz, ready):
    index = [lax.axis_index(name) for name in RING]
    size = [lax.axis_size(name) for name in RING]
    first_time = index[0] == 0
    last_time = index[0] == size[0] - 1
    first_z = index[1] == 0
    last_z = index[1] == size[1] - 1

    def no(condition):
        return jnp.logical_not(condition)

    def device(offset, back=False):
        return {
            RING[k]: lax.rem(index[k] + size[k] + (-step if back else step), size[k])
            for k, step in enumerate(offset)
            if step
        }

    barrier = pltpu.get_barrier_semaphore()

    def greet(offset):
        pl.semaphore_signal(barrier, inc=1, device_id=device(offset, back=True), device_id_type=MESH)

    fetch = [
        pltpu.make_async_copy(links_ref.at[pl.ds(mu * 18, 18)], u.at[pl.ds(mu * 18, 18)], in_sem.at[mu])
        for mu in range(4)
    ]
    for copy in fetch:
        copy.start()

    for offset in (DOWN[2], UP[2], CORNER_AT[1, 2]):
        greet(offset)
    pl.when(no(first_time))(lambda: greet(UP[0]))
    pl.when(no(first_z))(lambda: greet(UP[1]))
    pl.when(no(last_z))(lambda: greet(DOWN[1]))

    @pl.when(no(last_time))
    def _():
        for offset in (DOWN[0], CORNER_AT[1, 0], CORNER_AT[2, 0]):
            greet(offset)

    @pl.when(first_time)
    def _():
        for offset in (CORNER_AT[0, 1], CORNER_AT[0, 2]):
            greet(offset)

    for copy in fetch:
        copy.wait()

    def link(mu, part, i, j):
        return lambda: u[comp(mu, part, i, j)]

    for d in FACES:
        pack([link(nu, *c) for c in TWO_ROWS for nu in others(d) + [d]], send2[d], d, high=True)
    for number, (d, e) in enumerate(EDGES):
        pack_edge([link(d, *c) for c in TWO_ROWS], sende[number], d, e)
    for d in (1, 0, 2):
        pack([link(nu, *c) for nu in others(d) for c in TWO_ROWS], send1[d], d, high=False)

    middle = no(first_time | last_time)
    for here, count in ((first_time, 6), (middle, 9), (last_time, 11)):
        pl.when(here & first_z)(functools.partial(pl.semaphore_wait, barrier, count - 1))
        pl.when(here & no(first_z))(functools.partial(pl.semaphore_wait, barrier, count))
    pl.when(first_time)(lambda: greet(UP[0]))
    pl.when(first_z)(lambda: greet(UP[1]))
    pl.when(last_time)(lambda: greet(DOWN[0]))
    pl.when(last_z)(lambda: greet(DOWN[1]))

    @pl.when(no(first_time))
    def _():
        pl.semaphore_signal(ready, inc=1, device_id=device(DOWN[0]), device_id_type=MESH)

    def remote(src, dst, send, recv, offset):
        return pltpu.make_async_remote_copy(
            src_ref=src, dst_ref=dst, send_sem=send, recv_sem=recv,
            device_id=device(offset), device_id_type=MESH,
        )

    down = {d: remote(send1[d], recv1[d], s1.at[d], r1.at[d], DOWN[d]) for d in (0, 2)}
    parts_z = [
        remote(send1[1].at[pl.ds(3 * k, 3)], recv1[1].at[pl.ds(3 * k, 3)], sz.at[k], rz.at[k], DOWN[1])
        for k in range(3)
    ]
    up = [remote(send2[d], recv2[d], s2.at[d], r2.at[d], UP[d]) for d in range(3)]
    corner = {
        pair: remote(sende[n], recve[n], se.at[n], re.at[n], CORNER[n]) for n, pair in enumerate(EDGES)
    }
    def start(*copies):
        def body():
            for copy in copies:
                copy.start()

        return body

    corner[1, 2].start()
    pl.when(last_time)(start(corner[0, 1], corner[0, 2]))
    pl.when(no(first_time))(start(corner[1, 0], corner[2, 0]))
    down[2].start()
    up[0].start()
    pl.when(no(first_time))(down[0].start)
    up[1].start()
    pl.when(no(first_z))(start(*parts_z[::-1]))
    up[2].start()

    def second_stage():
        pl.when(first_time & first_z)(lambda: pl.semaphore_wait(barrier, 2))
        pl.when(first_time & no(first_z))(lambda: pl.semaphore_wait(barrier, 1))
        pl.when(no(first_time) & first_z)(lambda: pl.semaphore_wait(barrier, 1))
        pl.when(first_z)(corner[2, 1].start)
        pl.when(first_z & no(last_time))(corner[0, 1].start)
        pl.when(first_z)(start(*parts_z[::-1]))
        pl.when(first_time)(start(corner[1, 0], corner[2, 0], down[0]))

    def make_w(plane, mu, nu):
        def body(v, carry):
            rows = pl.ds(pl.multiple_of(v * 8, 8), 8)

            def get(ref, base):
                return [[(ref[base + i * 3 + j, rows, :], ref[base + 9 + i * 3 + j, rows, :])
                         for j in range(3)] for i in range(3)]

            a = get(u, mu * 18)
            b = get(u, nu * 18)
            for i in range(3):
                for j in range(3):
                    real, imag = dot3([(b[k][i], a[k][j]) for k in range(3)], conj_a=True)
                    wmat[plane * 18 + i * 3 + j, rows, :] = real
                    wmat[plane * 18 + 9 + i * 3 + j, rows, :] = imag
            return carry

        lax.fori_loop(0, 2, body, 0)

    def shift_x():
        for nu in others(3):
            at = slot(3, nu) * 18
            for c in range(18):
                shifted[at + c] = shift_within_x(u[nu * 18 + c])

    def shift_split(d, only=None):
        edge = position(d) == COUNT[d] - 1
        for order, nu in enumerate(others(d)):
            if only is not None and nu != only:
                continue
            at = slot(d, nu) * 18
            got = {}
            for number, (part, i, j) in enumerate(TWO_ROWS):
                local = turn(u[comp(nu, part, i, j)], d, -1)
                value = jnp.where(edge, unpack(recv1[d], order * 12 + number, d, high=True), local)
                got[part, i, j] = value
                shifted[at + part * 9 + i * 3 + j] = value

            def put(part, j, value, at=at):
                shifted[at + part * 9 + 6 + j] = value

            third_row(lambda *c: got[c], put)

    def face_near(d):
        where = position(d)
        for c in range(18):
            value = None
            for j, nu in enumerate(others(d)):
                part = turn(u[nu * 18 + c], d, j)
                value = part if value is None else jnp.where(where == j, part, value)
            near[d * 18 + c] = value

    def face_leaf(d):
        where = position(d)
        got_far, got_base, got_moved = {}, {}, {}
        per_tile = GROUP[d] // 4
        for number, c in enumerate(TWO_ROWS):
            value = turn(recv2[d][number // per_tile], d, -4 * (number % per_tile))
            got_far[c] = value
            spread = value
            for j in range(3):
                spread = jnp.where(where == j, turn(value, d, j - 3), spread)
            got_base[c] = spread
            shift = shift_within_x(spread)
            for j, mu in enumerate(others(d)):
                if mu == 3:
                    continue
                edge = EDGES.index((d, mu))
                step = jnp.where(
                    position(mu) == COUNT[mu] - 1,
                    unpack_edge(recve[edge], d, mu, number, j),
                    turn(spread, mu, -1),
                )
                shift = jnp.where(where == j, step, shift)
            got_moved[c] = shift
        for ref, got in ((far, got_far), (base, got_base), (moved, got_moved)):
            for (part, i, j), value in got.items():
                ref[part * 9 + i * 3 + j] = value

            def put(part, j, value, ref=ref):
                ref[part * 9 + 6 + j] = value

            third_row(lambda *c: got[c], put)

        def body(v, carry):
            rows = pl.ds(pl.multiple_of(v * 8, 8), 8)

            def get(ref, at, i, j):
                return (ref[at + i * 3 + j, rows, :], ref[at + 9 + i * 3 + j, rows, :])

            g = [[None] * 3 for _ in range(3)]
            for i in range(3):
                hi = [get(far, 0, i, k) for k in range(3)]
                for j in range(3):
                    g[i][j] = dot3([(hi[k], get(moved, 0, k, j)) for k in range(3)])
            x = [[None] * 3 for _ in range(3)]
            for i in range(3):
                ai = [get(near, d * 18, i, k) for k in range(3)]
                for j in range(3):
                    x[i][j] = dot3([(ai[k], g[j][k]) for k in range(3)], conj_b=True)

            def entry(i, j, parts):
                return dot3([(x[i][k], get(base, 0, k, j)) for k in range(3)], parts=parts)

            diag = [entry(i, i, "i")[1] for i in range(3)]
            trace = (diag[0] + diag[1] + diag[2]) * (1.0 / 3.0)
            values = leaf(lambda i, j, parts: (None, diag[i]) if i == j else entry(i, j, parts), trace)
            for c in range(8):
                faceleaf[c, rows, :] = values[c]
            return carry

        lax.fori_loop(0, 2, body, 0)

    def do_plane(plane, mu, nu):
        def body(v, carry):
            rows = pl.ds(pl.multiple_of(v * 8, 8), 8)

            def get(ref, base, i, j):
                return (ref[base + i * 3 + j, rows, :], ref[base + 9 + i * 3 + j, rows, :])

            cbase = slot(mu, nu) * 18
            dbase = slot(nu, mu) * 18
            t = [[None] * 3 for _ in range(3)]
            for i in range(3):
                ci = [get(shifted, cbase, i, k) for k in range(3)]
                for j in range(3):
                    t[i][j] = dot3([(ci[k], get(shifted, dbase, j, k)) for k in range(3)], conj_b=True)

            x = [[None] * 3 for _ in range(3)]
            for i in range(3):
                ai = [get(u, mu * 18, i, k) for k in range(3)]
                for j in range(3):
                    x[i][j] = dot3([(ai[k], t[k][j]) for k in range(3)])

            def p_entry(i, j, parts):
                return dot3([(x[i][k], get(u, nu * 18, j, k)) for k in range(3)], conj_b=True, parts=parts)

            diag = [p_entry(i, i, "i")[1] for i in range(3)]
            trace = (diag[0] + diag[1] + diag[2]) * (1.0 / 3.0)
            values = leaf(lambda i, j, parts: (None, diag[i]) if i == j else p_entry(i, j, parts), trace)
            for c in range(8):
                at_mu = (mu * 8 + c, rows, slice(None))
                at_nu = (nu * 8 + c, rows, slice(None))
                store[at_mu] = store[at_mu] + values[c]
                store[at_nu] = store[at_nu] - values[c]

            def w(i, j):
                return get(wmat, plane * 18, i, j)

            values = leaf(lambda i, j, parts: dot3([(w(i, k), t[k][j]) for k in range(3)], parts=parts), trace)
            for c in range(8):
                leaves[slot(nu, mu) * 8 + c, rows, :] = values[c]
            values = leaf(lambda i, j, parts: dot3([(t[i][k], w(k, j)) for k in range(3)], parts=parts), trace)
            for c in range(8):
                leaves[slot(mu, nu) * 8 + c, rows, :] = values[c]
            return carry

        lax.fori_loop(0, 2, body, 0)

    store[...] = jnp.zeros_like(store)
    shift_x()
    for plane, (mu, nu) in enumerate(PLANES):
        make_w(plane, mu, nu)
    for d in FACES:
        face_near(d)
    @pl.when(no(last_time))
    def _():
        pl.semaphore_wait(ready, 1)
        corner[0, 2].start()
        pl.when(no(first_z))(corner[0, 1].start)

    down[2].wait_recv()
    pl.when(no(first_z))(corner[2, 1].start)
    shift_split(2)
    do_plane(1, 2, 3)
    down[0].wait_recv()
    shift_split(0)
    do_plane(0, 0, 3)
    do_plane(2, 0, 2)

    def planes_z():
        for plane, nu in ((3, 3), (4, 2), (5, 0)):
            parts_z[others(1).index(nu)].wait_recv()
            shift_split(1, nu)
            do_plane(plane, *PLANES[plane])

    def face(d):
        up[d].wait_recv()
        for pair in EDGES:
            if pair[0] == d:
                corner[pair].wait_recv()
        face_leaf(d)
        first = position(d) == 0
        for order, nu in enumerate(others(d)):
            for c in range(8):
                store[nu * 8 + c] += jnp.where(first, turn(faceleaf[c], d, -order), 0.0)

    second_stage()
    stages = (planes_z, functools.partial(face, 2), functools.partial(face, 0), functools.partial(face, 1))
    orders = (
        (no(first_time | last_z), (0, 1, 2, 3)),
        (first_time & no(last_z), (0, 1, 3, 2)),
        (last_z & no(first_time), (3, 2, 1, 0)),
        (first_time & last_z, (3, 1, 0, 2)),
    )

    def take(step, carry):
        for number, stage in enumerate(stages):
            now = None
            for here, order in orders:
                hit = here & (step == order.index(number))
                now = hit if now is None else now | hit
            pl.when(now)(stage)
        return carry

    lax.fori_loop(0, len(stages), take, 0)

    for copy in list(down.values()) + parts_z + up + list(corner.values()):
        copy.wait_send()


def finish(store, leaves, out_ref, out, sem):
    def sign(d, nu):
        return -1 if (nu, d) in PLANES else 1

    def final(nu, c):
        value = store[nu * 8 + c]
        for d in others(nu):
            moved_leaf = leaves[slot(d, nu) * 8 + c]
            first = position(d) == 0
            if d == 3:
                around = pltpu.roll(moved_leaf, LANES - NX + 1, axis=1)
                moved_leaf = jnp.where(first, around, pltpu.roll(moved_leaf, 1, axis=1))
            else:
                moved_leaf = jnp.where(first, 0.0, turn(moved_leaf, d, 1))
            value = value + moved_leaf if sign(d, nu) > 0 else value - moved_leaf
        return value

    copies = []
    for mu in range(4):
        for number, (i, j) in enumerate(OFF):
            real = final(mu, number * 2) * (0.5 * COEFF)
            imag = final(mu, number * 2 + 1) * (0.5 * COEFF)
            out[comp(mu, 0, i, j)] = real
            out[comp(mu, 0, j, i)] = -real
            out[comp(mu, 1, i, j)] = imag
            out[comp(mu, 1, j, i)] = imag
        diag0 = final(mu, 6) * COEFF
        diag1 = final(mu, 7) * COEFF
        for i, value in enumerate((diag0, diag1, -(diag0 + diag1))):
            out[comp(mu, 1, i, i)] = value
            out[comp(mu, 0, i, i)] = jnp.zeros_like(value)
        part = pl.ds(mu * 18, 18)
        copies.append(pltpu.make_async_copy(out.at[part], out_ref.at[part], sem.at[mu]))
        copies[-1].start()
    for copy in copies:
        copy.wait()


def per_device(links):
    shape = links.shape
    vmem = pltpu.VMEM

    def packed(counts):
        return [vmem((n, ROWS, LANES), jnp.float32) for n in counts]

    counts1 = [-(-36 // g) for g in GROUP]
    counts2 = (12, 12, 6)
    edges = [vmem((ROWS, LANES), jnp.float32) for _ in EDGES]
    arrays = (72, 216, 108)
    dma = pltpu.SemaphoreType.DMA
    store, leaves = pl.pallas_call(
        kernel,
        out_shape=[jax.ShapeDtypeStruct((n, ROWS, LANES), jnp.float32) for n in (32, 96)],
        in_specs=[pl.BlockSpec(memory_space=pltpu.HBM)],
        out_specs=[pl.BlockSpec(memory_space=pltpu.VMEM)] * 2,
        scratch_shapes=packed(arrays)
        + [packed(counts1), packed(counts1), packed(counts2), packed(counts2), edges, edges]
        + packed((54, 18, 18, 18, 8))
        + [dma((n,)) for n in (4, 3, 3, 3, 3, 6, 6, 3, 3)] + [pltpu.SemaphoreType.REGULAR],
        compiler_params=pltpu.CompilerParams(
            collective_id=0, has_side_effects=True, vmem_limit_bytes=16 * 1024 * 1024
        ),
    )(pltpu.with_memory_space_constraint(links.reshape(72, ROWS, LANES), pltpu.HBM))
    out = pl.pallas_call(
        finish,
        out_shape=jax.ShapeDtypeStruct((72, ROWS, LANES), jnp.float32),
        in_specs=[pl.BlockSpec(memory_space=pltpu.VMEM)] * 2,
        out_specs=pl.BlockSpec(memory_space=pltpu.HBM),
        scratch_shapes=[vmem((72, ROWS, LANES), jnp.float32), dma((4,))],
        compiler_params=pltpu.CompilerParams(vmem_limit_bytes=16 * 1024 * 1024),
    )(store, leaves)
    return out.reshape(shape)


def solution(mesh):
    return jax.shard_map(
        per_device,
        mesh=mesh,
        in_specs=(P(None, None, None, None, "ta", "gz", "gx"),),
        out_specs=P(None, None, None, None, "ta", "gz", "gx"),
        check_vma=False,
    )
```
